32 devices in a mesh: tm: 8 (over z, y), space: 4 (over x, core).
Axes of the slice: x: 2, y: 2, z: 4, core: 2. Of those that a mesh axis runs over, the one named last changes fastest.
Arguments:
- states: float32 [8, 3, 256, 1024], P('tm', None, 'space'), may hold values from -3 to 3
- background: float32 [3, 256, 1024], P(None, 'space'), may hold values from -3 to 3
- obs_cells: int32 [8, 4, 1024], P('tm'), may hold values from 0 to 262143
- obs_values: float32 [8, 4, 1024], P('tm'), may hold values from -3 to 3
- land_mask: int32 [256, 1024], P('space'), may hold values 0 or 1
Outputs:
- gradient: float32 [8, 3, 256, 1024], P('tm', None, 'space')
- next_states: float32 [8, 3, 256, 1024], P('tm', None, 'space')
The draws below stay inside these ranges and needn't reach their ends.
All inputs are finite; a program needn't handle non-finite values. No bound on the sum of `land_mask` on one device may be relied on, other than what follows from the above.
Results may differ from the reference program's by a relative error of at most 0.0003.
Values sent between devices are 32-bit elements; how exact they have to be, the bound alone decides.
A program may use at most 64 MiB of HBM per device.

```python
import jax
import jax.numpy as jnp
from jax import lax

NLON = 1024
NSTEP = 4
OBS = 1024
NY = 256
SUBWIN = 8


def place_ends(array, rng, least, high):
    index_at = [jax.random.randint(jax.random.fold_in(rng, axis), (), 0, length) for axis, length in enumerate(array.shape)]
    main_axis = array.shape.index(max(array.shape))
    beside = index_at[:main_axis] + [(index_at[main_axis] + 1) % array.shape[main_axis]] + index_at[main_axis + 1:]
    return array.at[tuple(index_at)].set(least).at[tuple(beside)].set(high)


def shard_levels(key, extent, shards, least, top_value):
    def one(axis_at, blocks):
        steps = jax.random.uniform(jax.random.fold_in(jax.random.fold_in(key, 6), axis_at), (blocks,), jnp.float32, least / len(shards), top_value / len(shards))
        return jnp.repeat(jnp.exp(steps), extent[axis_at] // blocks).reshape((-1,) + (1,) * (len(extent) - axis_at - 1))

    factor_of = one(*shards[0])
    for cut in shards[1:]:
        factor_of = factor_of * one(*cut)
    return factor_of


def bell_draw(own_key, shape, width, reach, split=(), dtype=jnp.bfloat16):
    gain = shard_levels(own_key, shape, split, -0.22, 0.18) if split else 1.0
    array = jax.random.normal(own_key, shape, jnp.float32) * width * gain
    return jnp.minimum(jnp.maximum(array, -reach), reach).astype(dtype)


def setup_inputs(seed: int = 0) -> dict:
    arg_keys = jax.random.split(jax.random.key(seed), 6)
    states = bell_draw(arg_keys[0], (SUBWIN, 3, NY, NLON), 0.5, 3.0, ((0, 8), (2, 4)), jnp.float32)
    background = bell_draw(arg_keys[1], (3, NY, NLON), 0.5, 3.0, ((1, 4),), jnp.float32)
    obs_cells = place_ends(jax.random.randint(arg_keys[2], (SUBWIN, NSTEP, OBS), 0, NY * NLON), jax.random.fold_in(arg_keys[2], 1), 0, (NY * NLON) - 1).astype(jnp.int32)
    obs_values = bell_draw(arg_keys[3], (SUBWIN, NSTEP, OBS), 0.5, 3.0, ((0, 8),), jnp.float32)
    land_mask = place_ends((jax.random.randint(arg_keys[4], (NY, NLON), 0, 5) < 4).astype(jnp.int32), jax.random.fold_in(arg_keys[4], 1), 0, 1)
    return dict(states=states, background=background, obs_cells=obs_cells, obs_values=obs_values, land_mask=land_mask)


advect = 0.25
gravity = 1.0
coriolis = 0.1
diffuse = 0.1
defect_weight = 2.0
obs_weight = 4.0
step_length = 0.1

def along_lon(field):
    return (jnp.roll(field, -1, axis=-1) - jnp.roll(field, 1, axis=-1)) / 2.0

def advance(padded, land):
    height, zonal, merid = (padded[0], padded[1], padded[2])
    flux_x = (1.0 + height) * zonal
    flux_y = (1.0 + height) * merid

    def laplace(field):
        inner = field[1:-1]
        return field[2:] + field[:-2] + jnp.roll(inner, 1, axis=-1) + jnp.roll(inner, -1, axis=-1) - 4.0 * inner
    diverge = along_lon(flux_x)[1:-1] + (flux_y[2:] - flux_y[:-2]) / 2.0
    h_inner, u_inner, v_inner = (height[1:-1], zonal[1:-1], merid[1:-1])
    h_new = h_inner - advect * diverge + diffuse * laplace(height)
    u_new = land * (u_inner - advect * gravity * along_lon(height)[1:-1] + coriolis * v_inner + diffuse * laplace(zonal))
    v_new = land * (v_inner - advect * gravity * (height[2:] - height[:-2]) / 2.0 - coriolis * u_inner + diffuse * laplace(merid))
    return jnp.stack([h_new, u_new, v_new])

def subwindow(state, cells, values, land):
    current = state
    misfits = []
    for step in range(NSTEP):
        current = advance(jnp.pad(current, ((0, 0), (1, 1), (0, 0))), land)
        seen = jnp.take(current[0].reshape(-1), cells[step].astype(jnp.int32))
        misfits.append(seen - values[step])
    return (current, jnp.stack(misfits))

def reference(states, background, obs_cells, obs_values, land_mask):
    land = land_mask.astype(jnp.float32)
    ends = lax.map(lambda group: subwindow(group[0], group[1], group[2], land)[0], (states, obs_cells, obs_values))
    previous = jnp.concatenate([background[None], ends[:-1]], axis=0)
    defects = states - previous
    following = jnp.concatenate([defects[1:], jnp.zeros_like(defects[:1])], axis=0)

    def adjoint(group):
        state, cells, values, ahead = group
        outputs, pullback = jax.vjp(lambda s: subwindow(s, cells, values, land), state)
        return pullback((-defect_weight * ahead, obs_weight * outputs[1]))[0]
    gradient = defect_weight * defects + lax.map(adjoint, (states, obs_cells, obs_values, following))
    updated = states - step_length * gradient
    next_states = jnp.concatenate([updated[1:], ends[-1:]], axis=0)
    return (gradient, next_states)
```

```python
import functools

import jax
import jax.numpy as jnp
from jax import lax
from jax.experimental import pallas as pl
from jax.experimental.pallas import tpu as pltpu
from jax.sharding import PartitionSpec as P

NSTEP = 4
PAD = 8

advect = 0.25
gravity = 1.0
coriolis = 0.1
diffuse = 0.1
defect_weight = 2.0
obs_weight = 4.0
step_length = 0.1

KEEP = 1.0 - 4.0 * diffuse
HALF = advect / 2.0
HALF_G = advect * gravity / 2.0

MESH = pl.DeviceIdType.MESH


def kernel(
    n_tm,
    n_sp,
    states,
    background,
    cells,
    values,
    land,
    gradient,
    nexts,
    xt,
    yt,
    z0,
    prev_end,
    lam_a,
    lam_b,
    land_i,
    mask,
    dense_x,
    dense_y,
    cells_n,
    values_n,
    send,
    recv,
):
    rows, cols = states.shape[1], states.shape[2]
    tm, sp = lax.axis_index("tm"), lax.axis_index("space")
    wide = rows + 2 * PAD
    tiles = wide // PAD
    low, high = 2 * PAD, 2 * PAD + rows
    has_next, has_next2 = tm < n_tm - 1, tm < n_tm - 2
    has_prev, has_prev2 = tm > 0, tm > 1
    has_up, has_down = sp > 0, sp < n_sp - 1

    def span(t):
        return pl.ds(pl.multiple_of(t * PAD, PAD), PAD)

    for start in (0, PAD, high, high + PAD):
        blank = jnp.zeros((3, PAD, cols), jnp.float32)
        for ref in (xt.at[0], yt.at[0], z0):
            ref[:, start : start + PAD] = blank
        land_i[start : start + PAD] = jnp.zeros((PAD, cols), jnp.int32)

    barrier = pltpu.get_barrier_semaphore()
    near = (
        (has_up, (tm, sp - 1)),
        (has_down, (tm, sp + 1)),
        (has_prev, (tm - 1, sp)),
        (has_next, (tm + 1, sp)),
        (has_prev2, (tm - 2, sp)),
        (has_next2, (tm + 2, sp)),
    )
    for there, device in near:

        @pl.when(there)
        def _(device=device):
            pl.semaphore_signal(barrier, inc=1, device_id=device, device_id_type=MESH)

    pl.semaphore_wait(barrier, sum(there.astype(jnp.int32) for there, _ in near))

    def copy(index, src, dst, device):
        return pltpu.make_async_remote_copy(
            src_ref=src,
            dst_ref=dst,
            send_sem=send.at[index],
            recv_sem=recv.at[index],
            device_id=device,
            device_id_type=MESH,
        )

    started = []

    def start(index, src, dst, device, sends, receives):
        entry = copy(index, src, dst, device)

        @pl.when(sends)
        def _():
            entry.start()

        started.append((entry, sends))
        return entry, receives

    def arrive(*pairs):
        for entry, receives in pairs:

            @pl.when(receives)
            def _(entry=entry):
                entry.wait_recv()

    above, below = (tm, sp - 1), (tm, sp + 1)
    back, back2, ahead = (tm - 1, sp), (tm - 2, sp), (tm + 1, sp)
    yes_up, yes_down = has_up, has_down
    head, tail = pl.ds(0, PAD), pl.ds(rows - PAD, PAD)
    inner = pl.ds(PAD, rows - 2 * PAD)
    x0, y0 = xt.at[0], yt.at[0]
    top, bottom = pl.ds(PAD, PAD), pl.ds(high, PAD)
    y_head, y_tail = pl.ds(low, PAD), pl.ds(high - PAD, PAD)
    y_inner = pl.ds(low + PAD, rows - 2 * PAD)

    halo = [
        start(0, states.at[:, head], x0.at[:, bottom], above, yes_up, yes_down),
        start(1, states.at[:, tail], x0.at[:, top], below, yes_down, yes_up),
        start(2, land.at[head], land_i.at[bottom], above, yes_up, yes_down),
        start(3, land.at[tail], land_i.at[top], below, yes_down, yes_up),
    ]
    edges_y = [
        start(4, states.at[:, head], y0.at[:, y_head], back, has_prev, has_next),
        start(5, states.at[:, tail], y0.at[:, y_tail], back, has_prev, has_next),
    ]
    edges_z = [
        start(6, states.at[:, head], z0.at[:, y_head], back2, has_prev2, has_next2),
        start(7, states.at[:, tail], z0.at[:, y_tail], back2, has_prev2, has_next2),
    ]
    obs_next = [
        start(8, cells, cells_n, back, has_prev, has_next),
        start(9, values, values_n, back, has_prev, has_next),
    ]
    body_y = start(10, states.at[:, inner], y0.at[:, y_inner], back, has_prev, has_next)
    body_z = start(11, states.at[:, inner], z0.at[:, y_inner], back2, has_prev2, has_next2)

    first_row = sp * rows - PAD
    shift = cols.bit_length() - 1

    def densify(cells, values, dense):
        width = min(cols, 256)

        def one(s, carry):
            cell = cells[pl.ds(s, 1), :]
            value = values[pl.ds(s, 1), :]
            row = lax.shift_right_logical(cell, shift) - first_row
            col = lax.bitwise_and(cell, cols - 1)
            count = cell.shape[1]
            level = lax.broadcasted_iota(jnp.int32, (wide, count), 0)
            hit = level == row
            upper = value.astype(jnp.bfloat16).astype(jnp.float32)
            lower = value - upper
            picks = jnp.concatenate(
                [
                    jnp.where(hit, 1.0, 0.0),
                    jnp.where(hit, upper, 0.0),
                    jnp.where(hit, lower, 0.0),
                ],
                axis=0,
            ).astype(jnp.bfloat16)

            def part(c, carry):
                place = pl.multiple_of(c * width, width)
                column = lax.broadcasted_iota(jnp.int32, (width, count), 0) + place
                spread = jnp.where(column == col, 1.0, 0.0).astype(jnp.bfloat16)
                out = lax.dot_general(
                    picks, spread, (((1,), (1,)), ((), ())), preferred_element_type=jnp.float32
                )
                dense[s, 0, PAD : PAD + wide, pl.ds(place, width)] = obs_weight * out[:wide]
                dense[s, 1, PAD : PAD + wide, pl.ds(place, width)] = obs_weight * (
                    out[wide : 2 * wide] + out[2 * wide :]
                )
                return carry

            return lax.fori_loop(0, cols // width, part, carry)

        lax.fori_loop(0, NSTEP, one, 0)

    sub = lax.broadcasted_iota(jnp.int32, (PAD, cols), 0)
    is_first, is_last = sub == 0, sub == PAD - 1

    def valid(t):
        row = sub + (first_row + (t - 1) * PAD)
        return jnp.where((row >= 0) & (row < rows * n_sp), 1.0, 0.0)

    def around(ref, field, t):
        here = ref[field, span(t), :]
        before = ref[field, span(t - 1), :]
        after = ref[field, span(t + 1), :]
        up = pltpu.roll(jnp.where(is_last, before, here), 1, 0)
        down = pltpu.roll(jnp.where(is_first, after, here), PAD - 1, 0)
        left = pltpu.roll(here, 1, 1)
        right = pltpu.roll(here, cols - 1, 1)
        return here, up, down, left, right

    def forward(levels):
        def step(s, carry):
            src, dst = levels.at[s], levels.at[s + 1]

            def tile(t, carry):
                h, hu, hd, hl, hr = around(src, 0, t)
                u, uu, ud, ul, ur = around(src, 1, t)
                v, vu, vd, vl, vr = around(src, 2, t)
                m = mask[span(t), :]
                flux = (1.0 + hr) * ur - (1.0 + hl) * ul + (1.0 + hd) * vd - (1.0 + hu) * vu
                dst[0, span(t), :] = valid(t) * (
                    KEEP * h - HALF * flux + diffuse * ((hu + hd) + (hl + hr))
                )
                dst[1, span(t), :] = m * (
                    KEEP * u
                    - HALF_G * (hr - hl)
                    + coriolis * v
                    + diffuse * ((uu + ud) + (ul + ur))
                )
                dst[2, span(t), :] = m * (
                    KEEP * v
                    - HALF_G * (hd - hu)
                    - coriolis * u
                    + diffuse * ((vu + vd) + (vl + vr))
                )
                return carry

            return lax.fori_loop(1, tiles + 1, tile, carry)

        lax.fori_loop(0, NSTEP, step, 0)

    def begin(levels, following, there, dense, lam):
        def tile(t, carry):
            m = mask[span(t), :]
            ends = levels.at[NSTEP]

            def drive(field):
                defect = following[field, span(t), :] - ends[field, span(t), :]
                return jnp.where(there, -defect_weight * defect, 0.0)

            push = dense[NSTEP - 1, 0, span(t), :] * ends[0, span(t), :]
            push = push - dense[NSTEP - 1, 1, span(t), :]
            lam[0, span(t), :] = valid(t) * (drive(0) + push)
            lam[1, span(t), :] = m * drive(1)
            lam[2, span(t), :] = m * drive(2)
            return carry

        lax.fori_loop(1, tiles + 1, tile, 0)

    def adjoint_tile(src, state, t):
        p, pu, pd, pleft, pr = around(src, 0, t)
        q, qu, qd, ql, qr = around(src, 1, t)
        r, ru, rd, rl, rr = around(src, 2, t)
        depth = 1.0 + state[0, span(t), :]
        dx = HALF * (pr - pleft)
        dy = HALF * (pd - pu)
        lam_h = (
            KEEP * p
            + diffuse * ((pu + pd) + (pleft + pr))
            + state[1, span(t), :] * dx
            + state[2, span(t), :] * dy
            + HALF_G * ((qr - ql) + (rd - ru))
        )
        lam_u = KEEP * q + diffuse * ((qu + qd) + (ql + qr)) + depth * dx - coriolis * r
        lam_v = KEEP * r + diffuse * ((ru + rd) + (rl + rr)) + depth * dy + coriolis * q
        return lam_h, lam_u, lam_v

    def adjoint(levels, dense):
        src, dst = lam_a, lam_b
        for s in reversed(range(1, NSTEP)):

            def tile(t, carry, src=src, dst=dst, s=s):
                lam_h, lam_u, lam_v = adjoint_tile(src, levels.at[s], t)
                push = dense[s - 1, 0, span(t), :] * levels[s, 0, span(t), :]
                push = push - dense[s - 1, 1, span(t), :]
                m = mask[span(t), :]
                dst[0, span(t), :] = valid(t) * (lam_h + push)
                dst[1, span(t), :] = m * lam_u
                dst[2, span(t), :] = m * lam_v
                return carry

            lax.fori_loop(1, tiles + 1, tile, 0)
            src, dst = dst, src
        return src

    def place(t, carry):
        x0[:, span(t + 2), :] = states[:, span(t), :]
        land_i[span(t + 2), :] = land[span(t), :]
        return carry

    lax.fori_loop(0, rows // PAD, place, 0)
    densify(cells, values, dense_x)
    arrive(*halo)

    def to_mask(t, carry):
        mask[span(t), :] = land_i[span(t), :].astype(jnp.float32)
        return carry

    lax.fori_loop(0, tiles + 2, to_mask, 0)
    forward(xt)
    ends = start(
        12, xt.at[NSTEP, :, pl.ds(low, rows)], prev_end, ahead, has_next, has_prev
    )

    arrive(*edges_y)
    next_up = has_next & has_up
    next_down = has_next & has_down
    halo_y = [
        start(13, y0.at[:, y_head], y0.at[:, bottom], above, next_up, next_down),
        start(14, y0.at[:, y_tail], y0.at[:, top], below, next_down, next_up),
    ]
    arrive(*edges_z)
    next2_up = has_next2 & has_up
    next2_down = has_next2 & has_down
    halo_z = [
        start(15, z0.at[:, y_head], z0.at[:, bottom], above, next2_up, next2_down),
        start(16, z0.at[:, y_tail], z0.at[:, top], below, next2_down, next2_up),
    ]
    arrive(*obs_next)
    densify(cells_n, values_n, dense_y)
    arrive(body_y, *halo_y)

    begin(xt, y0, has_next, dense_x, lam_a)
    last = adjoint(xt, dense_x)

    def own(t, carry):
        lam = adjoint_tile(last, x0, t)
        for field in range(3):
            gradient[field, span(t - 2), :] = lam[field]
        return carry

    lax.fori_loop(2, tiles, own, 0)

    forward(yt)
    arrive(body_z, *halo_z)
    begin(yt, z0, has_next2, dense_y, lam_a)
    last = adjoint(yt, dense_y)

    def other(t, carry):
        lam = adjoint_tile(last, y0, t)
        for field in range(3):
            state = y0[field, span(t), :]
            end = xt[NSTEP, field, span(t), :]
            grad = defect_weight * (state - end) + lam[field]
            nexts[field, span(t - 2), :] = jnp.where(has_next, state - step_length * grad, end)
        return carry

    lax.fori_loop(2, tiles, other, 0)

    arrive(ends)

    def finish(t, carry):
        for field in range(3):
            before = jnp.where(
                has_prev, prev_end[field, span(t), :], background[field, span(t), :]
            )
            defect = states[field, span(t), :] - before
            gradient[field, span(t), :] = gradient[field, span(t), :] + defect_weight * defect
        return carry

    lax.fori_loop(0, rows // PAD, finish, 0)

    for entry, sends in started:

        @pl.when(sends)
        def _(entry=entry):
            entry.wait_send()


def solution(mesh):
    n_tm, n_sp = mesh.shape["tm"], mesh.shape["space"]

    def local(states, background, obs_cells, obs_values, land_mask):
        _, fields, rows, cols = states.shape
        padded = rows + 4 * PAD
        block = jax.ShapeDtypeStruct((fields, rows, cols), jnp.float32)
        f32 = functools.partial(pltpu.VMEM, dtype=jnp.float32)
        gradient, nexts = pl.pallas_call(
            functools.partial(kernel, n_tm, n_sp),
            out_shape=(block, block),
            in_specs=[pl.BlockSpec(memory_space=pltpu.VMEM)] * 5,
            out_specs=(pl.BlockSpec(memory_space=pltpu.VMEM),) * 2,
            scratch_shapes=[
                f32((NSTEP + 1, fields, padded, cols)),
                f32((NSTEP + 1, fields, padded, cols)),
                f32((fields, padded, cols)),
                f32((fields, rows, cols)),
                f32((fields, padded, cols)),
                f32((fields, padded, cols)),
                pltpu.VMEM((padded, cols), jnp.int32),
                f32((padded, cols)),
                f32((NSTEP, 2, padded, cols)),
                f32((NSTEP, 2, padded, cols)),
                pltpu.VMEM(obs_cells.shape[1:], jnp.int32),
                f32(obs_values.shape[1:]),
                pltpu.SemaphoreType.DMA((17,)),
                pltpu.SemaphoreType.DMA((17,)),
            ],
            compiler_params=pltpu.CompilerParams(
                collective_id=0, has_side_effects=True, vmem_limit_bytes=60 * 2**20
            ),
        )(states[0], background, obs_cells[0], obs_values[0], land_mask)
        return gradient[None], nexts[None]

    in_specs = (
        P("tm", None, "space", None),
        P(None, "space", None),
        P("tm", None, None),
        P("tm", None, None),
        P("space", None),
    )
    out_specs = (P("tm", None, "space", None), P("tm", None, "space", None))
    return jax.shard_map(local, mesh=mesh, in_specs=in_specs, out_specs=out_specs, check_vma=False)
```

```python
import functools

import jax
import jax.numpy as jnp
from jax import lax
from jax.experimental import pallas as pl
from jax.experimental.pallas import tpu as pltpu
from jax.sharding import PartitionSpec as P

NSTEP = 4
PAD = 8

advect = 0.25
gravity = 1.0
coriolis = 0.1
diffuse = 0.1
defect_weight = 2.0
obs_weight = 4.0
step_length = 0.1

KEEP = 1.0 - 4.0 * diffuse
HALF = advect / 2.0
HALF_G = advect * gravity / 2.0

MESH = pl.DeviceIdType.MESH


def kernel(
    n_tm,
    n_sp,
    states,
    background,
    cells,
    values,
    land,
    gradient,
    nexts,
    xt,
    yt,
    z0,
    prev_end,
    lam_a,
    lam_b,
    land_i,
    mask,
    dense_x,
    dense_y,
    cells_n,
    values_n,
    send,
    recv,
):
    rows, cols = states.shape[1], states.shape[2]
    tm, sp = lax.axis_index("tm"), lax.axis_index("space")
    wide = rows + 2 * PAD
    tiles = wide // PAD
    low, high = 2 * PAD, 2 * PAD + rows
    has_next, has_next2 = tm < n_tm - 1, tm < n_tm - 2
    has_prev, has_prev2 = tm > 0, tm > 1
    has_up, has_down = sp > 0, sp < n_sp - 1

    def span(t):
        return pl.ds(pl.multiple_of(t * PAD, PAD), PAD)

    for start in (0, PAD, high, high + PAD):
        blank = jnp.zeros((3, PAD, cols), jnp.float32)
        for ref in (xt.at[0], yt.at[0], z0):
            ref[:, start : start + PAD] = blank
        land_i[start : start + PAD] = jnp.zeros((PAD, cols), jnp.int32)

    barrier = pltpu.get_barrier_semaphore()
    near = (
        (has_up, (tm, sp - 1)),
        (has_down, (tm, sp + 1)),
        (has_prev, (tm - 1, sp)),
        (has_next, (tm + 1, sp)),
        (has_prev2, (tm - 2, sp)),
        (has_next2, (tm + 2, sp)),
    )
    for there, device in near:

        @pl.when(there)
        def _(device=device):
            pl.semaphore_signal(barrier, inc=1, device_id=device, device_id_type=MESH)

    pl.semaphore_wait(barrier, sum(there.astype(jnp.int32) for there, _ in near))

    def copy(index, src, dst, device):
        return pltpu.make_async_remote_copy(
            src_ref=src,
            dst_ref=dst,
            send_sem=send.at[index],
            recv_sem=recv.at[index],
            device_id=device,
            device_id_type=MESH,
        )

    started = []

    def start(index, src, dst, device, sends, receives):
        entry = copy(index, src, dst, device)

        @pl.when(sends)
        def _():
            entry.start()

        started.append((entry, sends))
        return entry, receives

    def arrive(*pairs):
        for entry, receives in pairs:

            @pl.when(receives)
            def _(entry=entry):
                entry.wait_recv()

    above, below = (tm, sp - 1), (tm, sp + 1)
    back, back2, ahead = (tm - 1, sp), (tm - 2, sp), (tm + 1, sp)
    yes_up, yes_down = has_up, has_down
    head, tail = pl.ds(0, PAD), pl.ds(rows - PAD, PAD)
    x0, y0 = xt.at[0], yt.at[0]
    top, bottom = pl.ds(PAD, PAD), pl.ds(high, PAD)
    y_head, y_tail = pl.ds(low, PAD), pl.ds(high - PAD, PAD)

    halo = [
        start(0, states.at[:, head], x0.at[:, bottom], above, yes_up, yes_down),
        start(1, states.at[:, tail], x0.at[:, top], below, yes_down, yes_up),
        start(2, land.at[head], land_i.at[bottom], above, yes_up, yes_down),
        start(3, land.at[tail], land_i.at[top], below, yes_down, yes_up),
    ]
    even = lax.rem(tm, 2) == 0
    odd = jnp.logical_not(even)
    obs_next = [
        start(4, cells, cells_n, back, has_prev, has_next),
        start(5, values, values_n, back, has_prev, has_next),
    ]
    pieces = [0, rows - PAD, *range(PAD, rows - PAD, PAD)]
    n_piece = len(pieces)
    source = [pl.ds(row, PAD) for row in pieces]
    target = [pl.ds(low + row, PAD) for row in pieces]
    far = [
        start(8 + i, states.at[:, source[i]], z0.at[:, target[i]], back2, has_prev2, has_next2)
        for i in range(n_piece)
    ]
    direct = [
        start(
            8 + n_piece + i,
            states.at[:, source[i]],
            y0.at[:, target[i]],
            back,
            odd,
            even & has_next,
        )
        for i in range(n_piece)
    ]
    relayed = []

    def relay(count):
        for i in range(len(relayed), min(len(relayed) + count, n_piece)):
            arrive(far[i])
            relayed.append(
                start(
                    8 + 2 * n_piece + i,
                    z0.at[:, target[i]],
                    y0.at[:, target[i]],
                    ahead,
                    even & has_next2,
                    odd & has_next,
                )
            )

    first_row = sp * rows - PAD
    shift = cols.bit_length() - 1

    def densify(cells, values, dense, begin_at, end_at):
        width = min(cols, 256)

        def one(s, carry):
            cell = cells[pl.ds(s, 1), :]
            value = values[pl.ds(s, 1), :]
            row = lax.shift_right_logical(cell, shift) - first_row
            col = lax.bitwise_and(cell, cols - 1)
            count = cell.shape[1]
            level = lax.broadcasted_iota(jnp.int32, (wide, count), 0)
            hit = level == row
            upper = value.astype(jnp.bfloat16).astype(jnp.float32)
            lower = value - upper
            picks = jnp.concatenate(
                [
                    jnp.where(hit, 1.0, 0.0),
                    jnp.where(hit, upper, 0.0),
                    jnp.where(hit, lower, 0.0),
                ],
                axis=0,
            ).astype(jnp.bfloat16)

            def part(c, carry):
                place = pl.multiple_of(c * width, width)
                column = lax.broadcasted_iota(jnp.int32, (width, count), 0) + place
                spread = jnp.where(column == col, 1.0, 0.0).astype(jnp.bfloat16)
                out = lax.dot_general(
                    picks, spread, (((1,), (1,)), ((), ())), preferred_element_type=jnp.float32
                )
                dense[s, 0, PAD : PAD + wide, pl.ds(place, width)] = obs_weight * out[:wide]
                dense[s, 1, PAD : PAD + wide, pl.ds(place, width)] = obs_weight * (
                    out[wide : 2 * wide] + out[2 * wide :]
                )
                return carry

            return lax.fori_loop(0, cols // width, part, carry)

        lax.fori_loop(begin_at, end_at, one, 0)

    sub = lax.broadcasted_iota(jnp.int32, (PAD, cols), 0)
    is_first, is_last = sub == 0, sub == PAD - 1

    def valid(t):
        row = sub + (first_row + (t - 1) * PAD)
        return jnp.where((row >= 0) & (row < rows * n_sp), 1.0, 0.0)

    def around(ref, field, t):
        here = ref[field, span(t), :]
        before = ref[field, span(t - 1), :]
        after = ref[field, span(t + 1), :]
        up = pltpu.roll(jnp.where(is_last, before, here), 1, 0)
        down = pltpu.roll(jnp.where(is_first, after, here), PAD - 1, 0)
        left = pltpu.roll(here, 1, 1)
        right = pltpu.roll(here, cols - 1, 1)
        return here, up, down, left, right

    def forward(levels):
        def step(s, carry):
            src, dst = levels.at[s], levels.at[s + 1]

            def tile(t, carry):
                h, hu, hd, hl, hr = around(src, 0, t)
                u, uu, ud, ul, ur = around(src, 1, t)
                v, vu, vd, vl, vr = around(src, 2, t)
                m = mask[span(t), :]
                flux = (1.0 + hr) * ur - (1.0 + hl) * ul + (1.0 + hd) * vd - (1.0 + hu) * vu
                dst[0, span(t), :] = valid(t) * (
                    KEEP * h - HALF * flux + diffuse * ((hu + hd) + (hl + hr))
                )
                dst[1, span(t), :] = m * (
                    KEEP * u
                    - HALF_G * (hr - hl)
                    + coriolis * v
                    + diffuse * ((uu + ud) + (ul + ur))
                )
                dst[2, span(t), :] = m * (
                    KEEP * v
                    - HALF_G * (hd - hu)
                    - coriolis * u
                    + diffuse * ((vu + vd) + (vl + vr))
                )
                return carry

            return lax.fori_loop(1, tiles + 1, tile, carry)

        lax.fori_loop(0, NSTEP, step, 0)

    def begin(levels, following, there, dense, lam):
        def tile(t, carry):
            m = mask[span(t), :]
            ends = levels.at[NSTEP]

            def drive(field):
                defect = following[field, span(t), :] - ends[field, span(t), :]
                return jnp.where(there, -defect_weight * defect, 0.0)

            push = dense[NSTEP - 1, 0, span(t), :] * ends[0, span(t), :]
            push = push - dense[NSTEP - 1, 1, span(t), :]
            lam[0, span(t), :] = valid(t) * (drive(0) + push)
            lam[1, span(t), :] = m * drive(1)
            lam[2, span(t), :] = m * drive(2)
            return carry

        lax.fori_loop(1, tiles + 1, tile, 0)

    def adjoint_tile(src, state, t):
        p, pu, pd, pleft, pr = around(src, 0, t)
        q, qu, qd, ql, qr = around(src, 1, t)
        r, ru, rd, rl, rr = around(src, 2, t)
        depth = 1.0 + state[0, span(t), :]
        dx = HALF * (pr - pleft)
        dy = HALF * (pd - pu)
        lam_h = (
            KEEP * p
            + diffuse * ((pu + pd) + (pleft + pr))
            + state[1, span(t), :] * dx
            + state[2, span(t), :] * dy
            + HALF_G * ((qr - ql) + (rd - ru))
        )
        lam_u = KEEP * q + diffuse * ((qu + qd) + (ql + qr)) + depth * dx - coriolis * r
        lam_v = KEEP * r + diffuse * ((ru + rd) + (rl + rr)) + depth * dy + coriolis * q
        return lam_h, lam_u, lam_v

    def adjoint(levels, dense):
        src, dst = lam_a, lam_b
        for s in reversed(range(1, NSTEP)):

            def tile(t, carry, src=src, dst=dst, s=s):
                lam_h, lam_u, lam_v = adjoint_tile(src, levels.at[s], t)
                push = dense[s - 1, 0, span(t), :] * levels[s, 0, span(t), :]
                push = push - dense[s - 1, 1, span(t), :]
                m = mask[span(t), :]
                dst[0, span(t), :] = valid(t) * (lam_h + push)
                dst[1, span(t), :] = m * lam_u
                dst[2, span(t), :] = m * lam_v
                return carry

            lax.fori_loop(1, tiles + 1, tile, 0)
            src, dst = dst, src
        return src

    def place(t, carry):
        x0[:, span(t + 2), :] = states[:, span(t), :]
        land_i[span(t + 2), :] = land[span(t), :]
        return carry

    lax.fori_loop(0, rows // PAD, place, 0)
    half = NSTEP // 2
    densify(cells, values, dense_x, 0, NSTEP)
    arrive(*halo)

    def to_mask(t, carry):
        mask[span(t), :] = land_i[span(t), :].astype(jnp.float32)
        return carry

    lax.fori_loop(0, tiles + 2, to_mask, 0)
    relay(2)
    forward(xt)
    relay(2)
    arrive(*obs_next)
    densify(cells_n, values_n, dense_y, 0, half)
    relay(1)
    densify(cells_n, values_n, dense_y, half, NSTEP)
    relay(1)
    arrive(*direct[:2], *relayed[:2])
    next_up = has_next & has_up
    next_down = has_next & has_down
    next2_up = has_next2 & has_up
    next2_down = has_next2 & has_down
    halo_next = [
        start(6, y0.at[:, y_head], y0.at[:, bottom], above, next_up, next_down),
        start(7, y0.at[:, y_tail], y0.at[:, top], below, next_down, next_up),
    ]
    base = 8 + 3 * n_piece
    halo_far = [
        start(base, z0.at[:, y_head], z0.at[:, bottom], above, next2_up, next2_down),
        start(base + 1, z0.at[:, y_tail], z0.at[:, top], below, next2_down, next2_up),
    ]
    relay(n_piece)
    arrive(*direct[2:], *relayed[2:])
    ends = start(
        base + 2, xt.at[NSTEP, :, pl.ds(low, rows)], prev_end, ahead, has_next, has_prev
    )
    arrive(*halo_next)

    begin(xt, y0, has_next, dense_x, lam_a)
    last = adjoint(xt, dense_x)

    def own(t, carry):
        lam = adjoint_tile(last, x0, t)
        for field in range(3):
            gradient[field, span(t - 2), :] = lam[field]
        return carry

    lax.fori_loop(2, tiles, own, 0)

    forward(yt)
    arrive(*halo_far)
    begin(yt, z0, has_next2, dense_y, lam_a)
    last = adjoint(yt, dense_y)

    def other(t, carry):
        lam = adjoint_tile(last, y0, t)
        for field in range(3):
            state = y0[field, span(t), :]
            end = xt[NSTEP, field, span(t), :]
            grad = defect_weight * (state - end) + lam[field]
            nexts[field, span(t - 2), :] = jnp.where(has_next, state - step_length * grad, end)
        return carry

    lax.fori_loop(2, tiles, other, 0)

    arrive(ends)

    def finish(t, carry):
        for field in range(3):
            before = jnp.where(
                has_prev, prev_end[field, span(t), :], background[field, span(t), :]
            )
            defect = states[field, span(t), :] - before
            gradient[field, span(t), :] = gradient[field, span(t), :] + defect_weight * defect
        return carry

    lax.fori_loop(0, rows // PAD, finish, 0)

    for entry, sends in started:

        @pl.when(sends)
        def _(entry=entry):
            entry.wait_send()


def solution(mesh):
    n_tm, n_sp = mesh.shape["tm"], mesh.shape["space"]

    def local(states, background, obs_cells, obs_values, land_mask):
        _, fields, rows, cols = states.shape
        padded = rows + 4 * PAD
        block = jax.ShapeDtypeStruct((fields, rows, cols), jnp.float32)
        f32 = functools.partial(pltpu.VMEM, dtype=jnp.float32)
        gradient, nexts = pl.pallas_call(
            functools.partial(kernel, n_tm, n_sp),
            out_shape=(block, block),
            in_specs=[pl.BlockSpec(memory_space=pltpu.VMEM)] * 5,
            out_specs=(pl.BlockSpec(memory_space=pltpu.VMEM),) * 2,
            scratch_shapes=[
                f32((NSTEP + 1, fields, padded, cols)),
                f32((NSTEP + 1, fields, padded, cols)),
                f32((fields, padded, cols)),
                f32((fields, rows, cols)),
                f32((fields, padded, cols)),
                f32((fields, padded, cols)),
                pltpu.VMEM((padded, cols), jnp.int32),
                f32((padded, cols)),
                f32((NSTEP, 2, padded, cols)),
                f32((NSTEP, 2, padded, cols)),
                pltpu.VMEM(obs_cells.shape[1:], jnp.int32),
                f32(obs_values.shape[1:]),
                pltpu.SemaphoreType.DMA((11 + 3 * (rows // PAD),)),
                pltpu.SemaphoreType.DMA((11 + 3 * (rows // PAD),)),
            ],
            compiler_params=pltpu.CompilerParams(
                collective_id=0, has_side_effects=True, vmem_limit_bytes=60 * 2**20
            ),
        )(states[0], background, obs_cells[0], obs_values[0], land_mask)
        return gradient[None], nexts[None]

    in_specs = (
        P("tm", None, "space", None),
        P(None, "space", None),
        P("tm", None, None),
        P("tm", None, None),
        P("space", None),
    )
    out_specs = (P("tm", None, "space", None), P("tm", None, "space", None))
    return jax.shard_map(local, mesh=mesh, in_specs=in_specs, out_specs=out_specs, check_vma=False)
```

```python
import functools

import jax
import jax.numpy as jnp
from jax import lax
from jax.experimental import pallas as pl
from jax.experimental.pallas import tpu as pltpu
from jax.sharding import PartitionSpec as P

NSTEP = 4
PAD = 8

advect = 0.25
gravity = 1.0
coriolis = 0.1
diffuse = 0.1
defect_weight = 2.0
obs_weight = 4.0
step_length = 0.1

KEEP = 1.0 - 4.0 * diffuse
HALF = advect / 2.0
HALF_G = advect * gravity / 2.0

MESH = pl.DeviceIdType.MESH


def kernel(
    n_tm,
    n_sp,
    states,
    background,
    cells,
    values,
    land,
    gradient,
    nexts,
    xt,
    yt,
    z0,
    prev_end,
    lam_a,
    lam_b,
    land_i,
    mask,
    dense_x,
    dense_y,
    cells_n,
    values_n,
    send,
    recv,
):
    rows, cols = states.shape[1], states.shape[2]
    tm, sp = lax.axis_index("tm"), lax.axis_index("space")
    wide = rows + 2 * PAD
    tiles = wide // PAD
    low, high = 2 * PAD, 2 * PAD + rows
    has_next, has_next2 = tm < n_tm - 1, tm < n_tm - 2
    has_prev, has_prev2 = tm > 0, tm > 1
    has_up, has_down = sp > 0, sp < n_sp - 1

    def span(t):
        return pl.ds(pl.multiple_of(t * PAD, PAD), PAD)

    for start in (0, PAD, high, high + PAD):
        blank = jnp.zeros((3, PAD, cols), jnp.float32)
        for ref in (xt.at[0], yt.at[0], z0):
            ref[:, start : start + PAD] = blank
        land_i[start : start + PAD] = jnp.zeros((PAD, cols), jnp.int32)

    barrier = pltpu.get_barrier_semaphore()
    near = (
        (has_up, (tm, sp - 1)),
        (has_down, (tm, sp + 1)),
        (has_prev, (tm - 1, sp)),
        (has_next, (tm + 1, sp)),
        (has_prev2, (tm - 2, sp)),
        (has_next2, (tm + 2, sp)),
    )
    for there, device in near:

        @pl.when(there)
        def _(device=device):
            pl.semaphore_signal(barrier, inc=1, device_id=device, device_id_type=MESH)

    pl.semaphore_wait(barrier, sum(there.astype(jnp.int32) for there, _ in near))

    def copy(index, src, dst, device):
        return pltpu.make_async_remote_copy(
            src_ref=src,
            dst_ref=dst,
            send_sem=send.at[index],
            recv_sem=recv.at[index],
            device_id=device,
            device_id_type=MESH,
        )

    started = []

    def start(index, src, dst, device, sends, receives):
        entry = copy(index, src, dst, device)

        @pl.when(sends)
        def _():
            entry.start()

        started.append((entry, sends))
        return entry, receives

    def arrive(*pairs):
        for entry, receives in pairs:

            @pl.when(receives)
            def _(entry=entry):
                entry.wait_recv()

    above, below = (tm, sp - 1), (tm, sp + 1)
    back, back2, ahead = (tm - 1, sp), (tm - 2, sp), (tm + 1, sp)
    yes_up, yes_down = has_up, has_down
    head, tail = pl.ds(0, PAD), pl.ds(rows - PAD, PAD)
    x0, y0 = xt.at[0], yt.at[0]
    top, bottom = pl.ds(PAD, PAD), pl.ds(high, PAD)
    y_head, y_tail = pl.ds(low, PAD), pl.ds(high - PAD, PAD)

    halo = [
        start(0, states.at[:, head], x0.at[:, bottom], above, yes_up, yes_down),
        start(1, states.at[:, tail], x0.at[:, top], below, yes_down, yes_up),
        start(2, land.at[head], land_i.at[bottom], above, yes_up, yes_down),
        start(3, land.at[tail], land_i.at[top], below, yes_down, yes_up),
    ]
    even = lax.rem(tm, 2) == 0
    odd = jnp.logical_not(even)
    obs_next = [
        start(4, cells, cells_n, back, has_prev, has_next),
        start(5, values, values_n, back, has_prev, has_next),
    ]
    pieces = [0, rows - PAD, *range(PAD, rows - PAD, PAD)]
    n_piece = len(pieces)
    source = [pl.ds(row, PAD) for row in pieces]
    target = [pl.ds(low + row, PAD) for row in pieces]
    far = [
        start(8 + i, states.at[:, source[i]], z0.at[:, target[i]], back2, has_prev2, has_next2)
        for i in range(n_piece)
    ]
    direct = [
        start(
            8 + n_piece + i,
            states.at[:, source[i]],
            y0.at[:, target[i]],
            back,
            odd,
            even & has_next,
        )
        for i in range(n_piece)
    ]
    relayed = []

    def relay(count):
        for i in range(len(relayed), min(len(relayed) + count, n_piece)):
            arrive(far[i])
            relayed.append(
                start(
                    8 + 2 * n_piece + i,
                    z0.at[:, target[i]],
                    y0.at[:, target[i]],
                    ahead,
                    even & has_next2,
                    odd & has_next,
                )
            )

    first_row = sp * rows - PAD
    shift = cols.bit_length() - 1

    def densify(cells, values, dense, begin_at, end_at):
        width = min(cols, 256)

        def one(s, carry):
            cell = cells[pl.ds(s, 1), :]
            value = values[pl.ds(s, 1), :]
            row = lax.shift_right_logical(cell, shift) - first_row
            col = lax.bitwise_and(cell, cols - 1)
            count = cell.shape[1]
            level = lax.broadcasted_iota(jnp.int32, (wide, count), 0)
            hit = level == row
            upper = value.astype(jnp.bfloat16).astype(jnp.float32)
            lower = value - upper
            picks = jnp.concatenate(
                [
                    jnp.where(hit, 1.0, 0.0),
                    jnp.where(hit, upper, 0.0),
                    jnp.where(hit, lower, 0.0),
                ],
                axis=0,
            ).astype(jnp.bfloat16)

            def part(c, carry):
                place = pl.multiple_of(c * width, width)
                column = lax.broadcasted_iota(jnp.int32, (width, count), 0) + place
                spread = jnp.where(column == col, 1.0, 0.0).astype(jnp.bfloat16)
                out = lax.dot_general(
                    picks, spread, (((1,), (1,)), ((), ())), preferred_element_type=jnp.float32
                )
                dense[s, 0, PAD : PAD + wide, pl.ds(place, width)] = obs_weight * out[:wide]
                dense[s, 1, PAD : PAD + wide, pl.ds(place, width)] = obs_weight * (
                    out[wide : 2 * wide] + out[2 * wide :]
                )
                return carry

            return lax.fori_loop(0, cols // width, part, carry)

        lax.fori_loop(begin_at, end_at, one, 0)

    sub = lax.broadcasted_iota(jnp.int32, (PAD, cols), 0)
    is_first, is_last = sub == 0, sub == PAD - 1

    def valid(t):
        row = sub + (first_row + (t - 1) * PAD)
        return jnp.where((row >= 0) & (row < rows * n_sp), 1.0, 0.0)

    def around(ref, field, t):
        here = ref[field, span(t), :]
        before = ref[field, span(t - 1), :]
        after = ref[field, span(t + 1), :]
        up = pltpu.roll(jnp.where(is_last, before, here), 1, 0)
        down = pltpu.roll(jnp.where(is_first, after, here), PAD - 1, 0)
        left = pltpu.roll(here, 1, 1)
        right = pltpu.roll(here, cols - 1, 1)
        return here, up, down, left, right

    def forward(levels):
        def step(s, carry):
            src, dst = levels.at[s], levels.at[s + 1]

            def tile(t, carry):
                h, hu, hd, hl, hr = around(src, 0, t)
                u, uu, ud, ul, ur = around(src, 1, t)
                v, vu, vd, vl, vr = around(src, 2, t)
                m = mask[span(t), :]
                flux = (1.0 + hr) * ur - (1.0 + hl) * ul + (1.0 + hd) * vd - (1.0 + hu) * vu
                dst[0, span(t), :] = valid(t) * (
                    KEEP * h - HALF * flux + diffuse * ((hu + hd) + (hl + hr))
                )
                dst[1, span(t), :] = m * (
                    KEEP * u
                    - HALF_G * (hr - hl)
                    + coriolis * v
                    + diffuse * ((uu + ud) + (ul + ur))
                )
                dst[2, span(t), :] = m * (
                    KEEP * v
                    - HALF_G * (hd - hu)
                    - coriolis * u
                    + diffuse * ((vu + vd) + (vl + vr))
                )
                return carry

            return lax.fori_loop(1, tiles + 1, tile, carry)

        lax.fori_loop(0, NSTEP, step, 0)

    def begin(levels, following, there, dense, lam):
        def tile(t, carry):
            m = mask[span(t), :]
            ends = levels.at[NSTEP]

            def drive(field):
                defect = following[field, span(t), :] - ends[field, span(t), :]
                return jnp.where(there, -defect_weight * defect, 0.0)

            push = dense[NSTEP - 1, 0, span(t), :] * ends[0, span(t), :]
            push = push - dense[NSTEP - 1, 1, span(t), :]
            lam[0, span(t), :] = valid(t) * (drive(0) + push)
            lam[1, span(t), :] = m * drive(1)
            lam[2, span(t), :] = m * drive(2)
            return carry

        lax.fori_loop(1, tiles + 1, tile, 0)

    def adjoint_tile(src, state, t):
        p, pu, pd, pleft, pr = around(src, 0, t)
        q, qu, qd, ql, qr = around(src, 1, t)
        r, ru, rd, rl, rr = around(src, 2, t)
        depth = 1.0 + state[0, span(t), :]
        dx = HALF * (pr - pleft)
        dy = HALF * (pd - pu)
        lam_h = (
            KEEP * p
            + diffuse * ((pu + pd) + (pleft + pr))
            + state[1, span(t), :] * dx
            + state[2, span(t), :] * dy
            + HALF_G * ((qr - ql) + (rd - ru))
        )
        lam_u = KEEP * q + diffuse * ((qu + qd) + (ql + qr)) + depth * dx - coriolis * r
        lam_v = KEEP * r + diffuse * ((ru + rd) + (rl + rr)) + depth * dy + coriolis * q
        return lam_h, lam_u, lam_v

    def adjoint(levels, dense):
        src, dst = lam_a, lam_b
        for s in reversed(range(1, NSTEP)):

            def tile(t, carry, src=src, dst=dst, s=s):
                lam_h, lam_u, lam_v = adjoint_tile(src, levels.at[s], t)
                push = dense[s - 1, 0, span(t), :] * levels[s, 0, span(t), :]
                push = push - dense[s - 1, 1, span(t), :]
                m = mask[span(t), :]
                dst[0, span(t), :] = valid(t) * (lam_h + push)
                dst[1, span(t), :] = m * lam_u
                dst[2, span(t), :] = m * lam_v
                return carry

            lax.fori_loop(1, tiles + 1, tile, 0)
            src, dst = dst, src
        return src

    def place(t, carry):
        x0[:, span(t + 2), :] = states[:, span(t), :]
        land_i[span(t + 2), :] = land[span(t), :]
        return carry

    lax.fori_loop(0, rows // PAD, place, 0)
    half = NSTEP // 2
    densify(cells, values, dense_x, 0, NSTEP)
    arrive(*halo)

    def to_mask(t, carry):
        mask[span(t), :] = land_i[span(t), :].astype(jnp.float32)
        return carry

    lax.fori_loop(0, tiles + 2, to_mask, 0)
    relay(2)
    forward(xt)
    relay(2)
    arrive(*obs_next)
    densify(cells_n, values_n, dense_y, 0, half)
    relay(1)
    densify(cells_n, values_n, dense_y, half, NSTEP)
    relay(1)
    arrive(*direct[:2], *relayed[:2])
    next_up = has_next & has_up
    next_down = has_next & has_down
    next2_up = has_next2 & has_up
    next2_down = has_next2 & has_down
    halo_next = [
        start(6, y0.at[:, y_head], y0.at[:, bottom], above, next_up, next_down),
        start(7, y0.at[:, y_tail], y0.at[:, top], below, next_down, next_up),
    ]
    base = 8 + 3 * n_piece
    halo_far = [
        start(base, z0.at[:, y_head], z0.at[:, bottom], above, next2_up, next2_down),
        start(base + 1, z0.at[:, y_tail], z0.at[:, top], below, next2_down, next2_up),
    ]
    relay(n_piece)
    ends = start(
        base + 2, xt.at[NSTEP, :, pl.ds(low, rows)], prev_end, ahead, has_next, has_prev
    )
    arrive(*direct[2:], *relayed[2:], *halo_next)

    begin(xt, y0, has_next, dense_x, lam_a)
    last = adjoint(xt, dense_x)

    def own(t, carry):
        lam = adjoint_tile(last, x0, t)
        for field in range(3):
            gradient[field, span(t - 2), :] = lam[field]
        return carry

    lax.fori_loop(2, tiles, own, 0)

    forward(yt)
    arrive(*halo_far)
    begin(yt, z0, has_next2, dense_y, lam_a)
    last = adjoint(yt, dense_y)

    def other(t, carry):
        lam = adjoint_tile(last, y0, t)
        for field in range(3):
            state = y0[field, span(t), :]
            end = xt[NSTEP, field, span(t), :]
            grad = defect_weight * (state - end) + lam[field]
            nexts[field, span(t - 2), :] = jnp.where(has_next, state - step_length * grad, end)
        return carry

    lax.fori_loop(2, tiles, other, 0)

    arrive(ends)

    def finish(t, carry):
        for field in range(3):
            before = jnp.where(
                has_prev, prev_end[field, span(t), :], background[field, span(t), :]
            )
            defect = states[field, span(t), :] - before
            gradient[field, span(t), :] = gradient[field, span(t), :] + defect_weight * defect
        return carry

    lax.fori_loop(0, rows // PAD, finish, 0)

    for entry, sends in started:

        @pl.when(sends)
        def _(entry=entry):
            entry.wait_send()


def solution(mesh):
    n_tm, n_sp = mesh.shape["tm"], mesh.shape["space"]

    def local(states, background, obs_cells, obs_values, land_mask):
        _, fields, rows, cols = states.shape
        padded = rows + 4 * PAD
        block = jax.ShapeDtypeStruct((fields, rows, cols), jnp.float32)
        f32 = functools.partial(pltpu.VMEM, dtype=jnp.float32)
        gradient, nexts = pl.pallas_call(
            functools.partial(kernel, n_tm, n_sp),
            out_shape=(block, block),
            in_specs=[pl.BlockSpec(memory_space=pltpu.VMEM)] * 5,
            out_specs=(pl.BlockSpec(memory_space=pltpu.VMEM),) * 2,
            scratch_shapes=[
                f32((NSTEP + 1, fields, padded, cols)),
                f32((NSTEP + 1, fields, padded, cols)),
                f32((fields, padded, cols)),
                f32((fields, rows, cols)),
                f32((fields, padded, cols)),
                f32((fields, padded, cols)),
                pltpu.VMEM((padded, cols), jnp.int32),
                f32((padded, cols)),
                f32((NSTEP, 2, padded, cols)),
                f32((NSTEP, 2, padded, cols)),
                pltpu.VMEM(obs_cells.shape[1:], jnp.int32),
                f32(obs_values.shape[1:]),
                pltpu.SemaphoreType.DMA((11 + 3 * (rows // PAD),)),
                pltpu.SemaphoreType.DMA((11 + 3 * (rows // PAD),)),
            ],
            compiler_params=pltpu.CompilerParams(
                collective_id=0, has_side_effects=True, vmem_limit_bytes=60 * 2**20
            ),
        )(states[0], background, obs_cells[0], obs_values[0], land_mask)
        return gradient[None], nexts[None]

    in_specs = (
        P("tm", None, "space", None),
        P(None, "space", None),
        P("tm", None, None),
        P("tm", None, None),
        P("space", None),
    )
    out_specs = (P("tm", None, "space", None), P("tm", None, "space", None))
    return jax.shard_map(local, mesh=mesh, in_specs=in_specs, out_specs=out_specs, check_vma=False)
```
